32 devices in a mesh: segment: 4 (over y, x), amp: 8 (over z, core).
Axes of the slice: x: 2, y: 2, z: 4, core: 2. Of those that a mesh axis runs over, the one named last changes fastest.
Arguments:
- states: float32 [4, 2097152], P('segment', 'amp'), may hold values from -6 to 6
- gate_blocks: float32 [4, 3, 128, 128], P('segment'), may hold values from -1 to 1, as said below
- kraus_picks: int32 [4, 4, 3, 7], P('segment'), may hold values from 0 to 3
- block_targets: int32 [4, 3], replicated, may hold values from 0 to 1
Outputs:
- final_states: float32 [4, 2097152], P('segment', 'amp')
- log_weights: float32 [4, 4], P('segment')
The draws below stay inside these ranges and needn't reach their ends.
Inputs may be any that keep to these rules, and one draw needn't show every extreme that they name: Every block of gate_blocks is an orthogonal matrix, up to rounding.
All inputs are finite; a program needn't handle non-finite values.
Results may differ from the reference program's by a relative error of at most 0.0003.
Values sent between devices are 32-bit elements; how exact they have to be, the bound alone decides.
A program may use at most 64 MiB of HBM per device.

```python
import jax
import jax.numpy as jnp
from jax import lax

QB = 7
REG = 128
MIDC = 16
BLOCKS = 3
SECTIONS = 4
TRAJ = 4
GLOBALS = 8
AMPS = 2097152


def draw_gate_blocks(key, part):
    gaussian = jax.random.normal(key, (SECTIONS, BLOCKS, REG, REG), jnp.float32)
    q_factor, r_factor = jnp.linalg.qr(gaussian)
    return q_factor.astype(jnp.float32)


def place_ends(array, key, low, largest):
    place = [jax.random.randint(jax.random.fold_in(key, axis), (), 0, length) for axis, length in enumerate(array.shape)]
    main_axis = array.shape.index(max(array.shape))
    beside = place[:main_axis] + [(place[main_axis] + 1) % array.shape[main_axis]] + place[main_axis + 1:]
    return array.at[tuple(place)].set(low).at[tuple(beside)].set(largest)


def level_of(rng, extent, shards, smallest, largest):
    factor_of = 1.0
    for axis_at, shards_of in shards:
        heights = jax.random.uniform(jax.random.fold_in(jax.random.fold_in(rng, 6), axis_at), (shards_of,), jnp.float32, smallest / len(shards), largest / len(shards))
        factor_of = factor_of * jnp.repeat(jnp.exp(heights), extent[axis_at] // shards_of).reshape((-1,) + (1,) * (len(extent) - 1 - axis_at))
    return factor_of


def normal_values(own_key, extent, deviation, most, cuts=(), kind=jnp.bfloat16):
    gain = level_of(own_key, extent, cuts, -0.22, 0.18) if cuts else 1.0
    values = jax.random.normal(own_key, extent, jnp.float32) * deviation * gain
    return jnp.minimum(jnp.maximum(values, -most), most).astype(kind)


def setup_inputs(seed: int = 0) -> dict:
    arg_keys = jax.random.split(jax.random.key(seed), 5)
    states = normal_values(arg_keys[0], (TRAJ, AMPS), 1.0, 6.0, ((0, 4), (1, 8)), jnp.float32)
    gate_blocks = draw_gate_blocks(jax.random.fold_in(arg_keys[4], 71), 0)
    kraus_picks = place_ends(jax.random.randint(arg_keys[2], (TRAJ, SECTIONS, BLOCKS, QB), 0, 4), jax.random.fold_in(arg_keys[2], 1), 0, 3).astype(jnp.int32)
    block_targets = place_ends(jax.random.randint(arg_keys[3], (SECTIONS, BLOCKS), 0, 2), jax.random.fold_in(arg_keys[3], 1), 0, 1).astype(jnp.int32)
    return {"states": states, "gate_blocks": gate_blocks, "kraus_picks": kraus_picks, "block_targets": block_targets}


KEEP_FACTORS = (1.0, 0.9, 1.0, 0.97)
FLIP_FACTORS = (0.9, 1.0, 0.97, 1.0)

def noise_factors(kraus_rows):
    qubit_count = kraus_rows.shape[-1]
    register = 2 ** qubit_count
    positions = jnp.arange(register, dtype=jnp.int32)
    product = jnp.ones(kraus_rows.shape[:-1] + (register,), jnp.float32)
    for qubit_pos in range(qubit_count):
        bit_value = jnp.right_shift(positions, qubit_count - 1 - qubit_pos) & 1
        column = kraus_rows[..., qubit_pos:qubit_pos + 1]
        low_value = jnp.zeros(column.shape, jnp.float32)
        high_value = jnp.zeros(column.shape, jnp.float32)
        for option in range(4):
            picked = (column == option).astype(jnp.float32)
            low_value = low_value + picked * KEEP_FACTORS[option]
            high_value = high_value + picked * FLIP_FACTORS[option]
        product = product * jnp.where(bit_value == 1, high_value, low_value)
    return product

def apply_gate(amplitudes, matrix, factors, target):

    def on_low(values):
        mixed_rows = jnp.einsum('bghmk,ik->bghmi', values, matrix, precision=lax.Precision.HIGHEST)
        return mixed_rows * factors[:, None, None, None, :]

    def on_high(values):
        mixed_rows = jnp.einsum('bgjmk,ij->bgimk', values, matrix, precision=lax.Precision.HIGHEST)
        return mixed_rows * factors[:, None, :, None, None]
    return lax.cond(target == 0, on_low, on_high, amplitudes)

def swap_global(amplitudes):
    traj_all, global_count, register, middle, low_count = amplitudes.shape
    split_view = amplitudes.reshape(traj_all, global_count, global_count, register // global_count, middle, low_count)
    swapped = jnp.swapaxes(split_view, 1, 2)
    return swapped.reshape(traj_all, global_count, register, middle, low_count)

def reference(states, gate_blocks, kraus_picks, block_targets):
    register = gate_blocks.shape[-1]
    amplitudes = states.reshape(TRAJ, GLOBALS, register, MIDC, register)
    mean_sq = lax.optimization_barrier(jnp.mean(amplitudes * amplitudes, axis=(1, 2, 3, 4)))
    amplitudes = amplitudes / jnp.sqrt(mean_sq)[:, None, None, None, None]
    log_list = []
    for section in range(SECTIONS):
        for block_pos in range(BLOCKS):
            factors = noise_factors(kraus_picks[:, section, block_pos, :])
            amplitudes = apply_gate(amplitudes, gate_blocks[section, block_pos], factors, block_targets[section, block_pos])
        amplitudes = swap_global(amplitudes)
        mean_sq = lax.optimization_barrier(jnp.mean(amplitudes * amplitudes, axis=(1, 2, 3, 4)))
        log_list.append(jnp.log(mean_sq))
        amplitudes = amplitudes / jnp.sqrt(mean_sq)[:, None, None, None, None]
    return (amplitudes.reshape(TRAJ, AMPS), jnp.stack(log_list, axis=1))
```

```python
import functools

import jax
import jax.numpy as jnp
from jax import lax
from jax.experimental import pallas as pl
from jax.experimental.pallas import tpu as pltpu
from jax.sharding import PartitionSpec as P

KEEP_FACTORS = (1.0, 0.9, 1.0, 0.97)
FLIP_FACTORS = (0.9, 1.0, 0.97, 1.0)
MESH = pl.DeviceIdType.MESH


def broadcast(block, axis, owner):
    block = jnp.where(lax.axis_index(axis) == owner, block, jnp.zeros_like(block))
    return lax.psum(block, axis)


def noise_factors(kraus_rows):
    qubit_count = kraus_rows.shape[-1]
    register = 2**qubit_count
    positions = jnp.arange(register, dtype=jnp.int32)
    product = jnp.ones(kraus_rows.shape[:-1] + (register,), jnp.float32)
    for qubit_pos in range(qubit_count):
        bit_value = jnp.right_shift(positions, qubit_count - 1 - qubit_pos) & 1
        column = kraus_rows[..., qubit_pos : qubit_pos + 1]
        low_value = jnp.zeros(column.shape, jnp.float32)
        high_value = jnp.zeros(column.shape, jnp.float32)
        for option in range(4):
            picked = (column == option).astype(jnp.float32)
            low_value = low_value + picked * KEEP_FACTORS[option]
            high_value = high_value + picked * FLIP_FACTORS[option]
        product = product * jnp.where(bit_value == 1, high_value, low_value)
    return product


def apply_gate(amplitudes, matrix, factors, target):

    def on_low(values):
        mixed_rows = jnp.einsum("bhmk,ik->bhmi", values, matrix, precision=lax.Precision.HIGHEST)
        return mixed_rows * factors[:, None, None, :]

    def on_high(values):
        mixed_rows = jnp.einsum("bjmk,ij->bimk", values, matrix, precision=lax.Precision.HIGHEST)
        return mixed_rows * factors[:, :, None, None]

    return lax.cond(target == 0, on_low, on_high, amplitudes)


def square_sums(values):
    return (values, jnp.sum(values * values, axis=(1, 2, 3)))


def body(states, gate_blocks, kraus_picks, block_targets):
    traj_here = states.shape[0]
    amp_local = states.shape[1]
    register = gate_blocks.shape[-1]
    blocks = gate_blocks.shape[1]
    middle = amp_local // (register * register)
    total_amps = amp_local * lax.axis_size("amp")
    sections = lax.axis_size("segment")
    amplitudes = states.reshape(traj_here, register, middle, register)
    first_local = jnp.sum(amplitudes * amplitudes, axis=(1, 2, 3))
    local_sums = [first_local]
    for section in range(sections):
        section_gates = broadcast(gate_blocks, "segment", section)[0]
        for block_pos in range(blocks):
            factors = noise_factors(kraus_picks[:, section, block_pos, :])
            amplitudes = apply_gate(
                amplitudes, section_gates[block_pos], factors, block_targets[section, block_pos]
            )
        amplitudes, local_sq = square_sums(
            lax.all_to_all(amplitudes, "amp", split_axis=1, concat_axis=1, tiled=True)
        )
        local_sums.append(local_sq)
    totals = lax.psum(jnp.stack(local_sums, axis=1), "amp")
    log_weights = jnp.log(totals[:, 1:] / totals[:, :-1])
    amplitudes = amplitudes / jnp.sqrt(totals[:, -1] / total_amps)[:, None, None, None]
    return (amplitudes.reshape(traj_here, amp_local), log_weights)


def partner(index, k):
    result = index
    bit = 1
    while bit <= k:
        if k & bit:
            result = result + bit * (1 - 2 * ((index // bit) % 2))
        bit *= 2
    return result


def split(values):
    high = values.astype(jnp.bfloat16)
    low = (values - high.astype(jnp.float32)).astype(jnp.bfloat16)
    return high, low


def left_form(matrix):
    return jnp.concatenate(split(matrix), axis=1)


def right_form(matrix):
    row = jnp.concatenate(split(matrix), axis=1)
    return jnp.concatenate([row, row], axis=0)


def multiply(left, right):
    both = jnp.dot(left, right, preferred_element_type=jnp.float32)
    half = both.shape[1] // 2
    return both[:, :half] + both[:, half:]


def fold_rows(values):
    squares = values * values
    return jnp.sum(squares.reshape(-1, 8, squares.shape[-1]), axis=0)


def row_factors(picks_ref, row, qubits, shape):
    positions = lax.broadcasted_iota(jnp.int32, shape, 0)
    product = jnp.ones(shape, jnp.float32)
    for q in range(qubits):
        pick = picks_ref[row * qubits + q]
        keep = jnp.float32(KEEP_FACTORS[0])
        flip = jnp.float32(FLIP_FACTORS[0])
        for option in range(1, 4):
            keep = jnp.where(pick == option, jnp.float32(KEEP_FACTORS[option]), keep)
            flip = jnp.where(pick == option, jnp.float32(FLIP_FACTORS[option]), flip)
        bit = jnp.right_shift(positions, qubits - 1 - q) & 1
        product = product * jnp.where(bit == 1, flip, keep)
    return product


def circuit_kernel(
    peers, sections, blocks, qubits, chunks, total_amps,
    x_hbm, gates_hbm, picks_ref, targets_ref,
    out_ref, logs_ref,
    xs, yin, ov, gates, low_form, high_form, partial, sums,
    x_sem, own_sem, gate_sem, gsend, grecv, isend, irecv, osend, orecv, ssend, srecv,
):
    seg = lax.axis_index("segment")
    amp = lax.axis_index("amp")
    reg = gates.shape[-1]
    middle = chunks * peers
    order = list(range(peers - 1, 0, -1))

    loads = []
    for chunk in range(chunks):
        for d in range(peers):
            m = chunk * peers + d
            load = pltpu.make_async_copy(x_hbm.at[:, m, 0], xs.at[m], x_sem.at[m])
            load.start()
            loads.append(load)
    gate_load = pltpu.make_async_copy(gates_hbm, gates.at[seg], gate_sem)
    gate_load.start()
    own_loads = []
    for chunk in range(chunks):
        own = pltpu.make_async_copy(
            x_hbm.at[:, chunk * peers + amp, 0], yin.at[chunk, amp], own_sem.at[chunk]
        )
        own.start()
        own_loads.append(own)

    barrier = pltpu.get_barrier_semaphore()
    for k in order:
        pl.semaphore_signal(
            barrier, inc=1, device_id={"amp": partner(amp, k)}, device_id_type=MESH
        )
    for k in range(1, sections):
        pl.semaphore_signal(
            barrier, inc=1, device_id={"segment": partner(seg, k)}, device_id_type=MESH
        )
    pl.semaphore_wait(barrier, peers - 1 + sections - 1)

    for load in loads:
        load.wait()

    in_copies = []
    for chunk in range(chunks):
        copies = []
        for k in order:
            peer = partner(amp, k)
            copy = pltpu.make_async_remote_copy(
                src_ref=xs.at[chunk * peers + peer],
                dst_ref=yin.at[chunk, amp],
                send_sem=isend.at[chunk, k],
                recv_sem=irecv.at[chunk, k],
                device_id={"amp": peer},
                device_id_type=MESH,
            )
            copy.start()
            copies.append(copy)
        in_copies.append(copies)

    gate_load.wait()
    gate_copies = []
    for k in range(1, sections):
        copy = pltpu.make_async_remote_copy(
            src_ref=gates.at[seg],
            dst_ref=gates.at[seg],
            send_sem=gsend.at[k],
            recv_sem=grecv.at[k],
            device_id={"segment": partner(seg, k)},
            device_id_type=MESH,
        )
        copy.start()
        gate_copies.append(copy)
    for copy in gate_copies:
        copy.wait_recv()

    rows_at = lax.broadcasted_iota(jnp.int32, (reg, reg), 0)
    columns_at = lax.broadcasted_iota(jnp.int32, (reg, reg), 1)
    identity = jnp.where(rows_at == columns_at, jnp.float32(1.0), jnp.float32(0.0))

    def build(section, carry):
        low = high = None
        for b in range(blocks):
            row = section * blocks + b
            damped = gates[section, b] * row_factors(picks_ref, row, qubits, (reg, reg))
            is_low = targets_ref[row] == 0
            for_low = jnp.where(is_low, damped, identity)
            for_high = jnp.where(is_low, identity, damped)
            if b == 0:
                low, high = for_low, for_high
            else:
                low = multiply(left_form(for_low), right_form(low))
                high = multiply(left_form(for_high), right_form(high))
        low_form[section] = right_form(low.T)
        high_form[section] = left_form(high)
        return carry

    lax.fori_loop(0, sections, build, 0)

    inner = reg // peers
    partial[...] = jnp.zeros_like(partial)

    def apply_section(chunk, section, swapped):
        low = low_form[section]
        high = high_form[section]
        total = jnp.zeros((8, reg), jnp.float32)
        for slab in range(peers):
            if swapped:
                value = yin[chunk, :, slab * inner : (slab + 1) * inner, :].reshape(reg, reg)
            else:
                value = yin[chunk, slab]
            value = multiply(left_form(value), low)
            value = multiply(high, right_form(value))
            total = total + fold_rows(value)
            if swapped:
                yin[chunk, :, slab * inner : (slab + 1) * inner, :] = value.reshape(
                    peers, inner, reg
                )
            else:
                yin[chunk, slab] = value
        partial[section + 1] = partial[section + 1] + total

    out_copies = []
    for chunk in range(chunks):
        own_loads[chunk].wait()
        for copy in in_copies[chunk]:
            copy.wait_recv()
        first = jnp.zeros((8, reg), jnp.float32)
        for slab in range(peers):
            first = first + fold_rows(yin[chunk, slab])
        partial[0] = partial[0] + first

        def pair(i, carry, chunk=chunk):
            apply_section(chunk, 2 * i, False)
            apply_section(chunk, 2 * i + 1, True)
            return carry

        lax.fori_loop(0, sections // 2, pair, 0)

        if chunk == chunks - 1:
            for s in range(sections + 1):
                sums[amp, s : s + 1, :] = jnp.sum(partial[s], axis=0, keepdims=True)
            sum_copies = []
            for k in order:
                copy = pltpu.make_async_remote_copy(
                    src_ref=sums.at[amp],
                    dst_ref=sums.at[amp],
                    send_sem=ssend.at[k],
                    recv_sem=srecv.at[k],
                    device_id={"amp": partner(amp, k)},
                    device_id_type=MESH,
                )
                copy.start()
                sum_copies.append(copy)
        copies = []
        for k in order:
            peer = partner(amp, k)
            copy = pltpu.make_async_remote_copy(
                src_ref=yin.at[chunk, peer],
                dst_ref=ov.at[chunk, amp],
                send_sem=osend.at[chunk, k],
                recv_sem=orecv.at[chunk, k],
                device_id={"amp": peer},
                device_id_type=MESH,
            )
            copy.start()
            copies.append(copy)
        out_copies.append(copies)

    for copy in sum_copies:
        copy.wait_recv()
    totals = []
    for s in range(sections + 1):
        total = sums[0, s : s + 1, :]
        for d in range(1, peers):
            total = total + sums[d, s : s + 1, :]
        totals.append(jnp.sum(total, axis=1, keepdims=True))
    lanes = lax.broadcasted_iota(jnp.int32, (1, reg), 1)
    logs = jnp.zeros((1, reg), jnp.float32)
    for s in range(sections):
        logs = jnp.where(lanes == s, jnp.log(totals[s + 1] / totals[s]), logs)
    logs_ref[...] = logs[:, :sections]
    scale = 1.0 / jnp.sqrt(totals[sections] / total_amps)
    scale = jnp.broadcast_to(scale, (1, reg))

    for chunk in range(chunks):
        m = chunk * peers + amp
        out_ref[pl.ds(m, reg, stride=middle), :] = yin[chunk, amp] * scale
    for chunk in range(chunks):
        for at, k in reversed(list(enumerate(order))):
            out_copies[chunk][at].wait_recv()
            m = chunk * peers + partner(amp, k)
            out_ref[pl.ds(m, reg, stride=middle), :] = ov[chunk, partner(amp, k)] * scale

    for copies in in_copies + out_copies + [gate_copies, sum_copies]:
        for copy in copies:
            copy.wait_send()


def step(states, gate_blocks, kraus_picks, block_targets):
    traj_here, amp_local = states.shape
    reg = gate_blocks.shape[-1]
    blocks = gate_blocks.shape[1]
    qubits = kraus_picks.shape[-1]
    peers = lax.axis_size("amp")
    sections = lax.axis_size("segment")
    middle = amp_local // (reg * reg)
    fits = (
        traj_here == 1
        and gate_blocks.shape[0] == 1
        and middle % peers == 0
        and peers & (peers - 1) == 0
        and sections & (sections - 1) == 0
        and sections % 2 == 0
        and sections < 8
        and reg == 128
        and reg % (8 * peers) == 0
    )
    if not fits:
        return body(states, gate_blocks, kraus_picks, block_targets)
    chunks = middle // peers
    kernel = functools.partial(
        circuit_kernel, peers, sections, blocks, qubits, chunks, amp_local * peers
    )
    f32 = jnp.float32
    dma = pltpu.SemaphoreType.DMA
    out, logs = pl.pallas_call(
        kernel,
        out_shape=(
            jax.ShapeDtypeStruct((reg * middle, reg), f32),
            jax.ShapeDtypeStruct((1, sections), f32),
        ),
        in_specs=[
            pl.BlockSpec(memory_space=pl.ANY),
            pl.BlockSpec(memory_space=pl.ANY),
            pl.BlockSpec(memory_space=pltpu.SMEM),
            pl.BlockSpec(memory_space=pltpu.SMEM),
        ],
        out_specs=(
            pl.BlockSpec(memory_space=pltpu.VMEM),
            pl.BlockSpec(memory_space=pltpu.VMEM),
        ),
        scratch_shapes=[
            pltpu.VMEM((middle, reg, reg), f32),
            pltpu.VMEM((chunks, peers, reg, reg), f32),
            pltpu.VMEM((chunks, peers, reg, reg), f32),
            pltpu.VMEM((sections, blocks, reg, reg), f32),
            pltpu.VMEM((sections, 2 * reg, 2 * reg), jnp.bfloat16),
            pltpu.VMEM((sections, reg, 2 * reg), jnp.bfloat16),
            pltpu.VMEM((sections + 1, 8, reg), f32),
            pltpu.VMEM((peers, 8, reg), f32),
            dma((middle,)),
            dma((chunks,)),
            dma,
            dma((sections,)),
            dma((sections,)),
            dma((chunks, peers)),
            dma((chunks, peers)),
            dma((chunks, peers)),
            dma((chunks, peers)),
            dma((peers,)),
            dma((peers,)),
        ],
        compiler_params=pltpu.CompilerParams(collective_id=0, has_side_effects=True),
    )(
        states.reshape(reg, middle, 1, reg),
        gate_blocks[0],
        kraus_picks.reshape(-1),
        block_targets.reshape(-1),
    )
    return out.reshape(1, amp_local), logs


def solution(mesh):
    in_specs = (
        P("segment", "amp"),
        P("segment", None, None, None),
        P("segment", None, None, None),
        P(),
    )
    out_specs = (P("segment", "amp"), P("segment", None))
    return jax.shard_map(step, mesh=mesh, in_specs=in_specs, out_specs=out_specs, check_vma=False)
```

```python
import functools

import jax
import jax.numpy as jnp
from jax import lax
from jax.experimental import pallas as pl
from jax.experimental.pallas import tpu as pltpu
from jax.sharding import PartitionSpec as P

KEEP_FACTORS = (1.0, 0.9, 1.0, 0.97)
FLIP_FACTORS = (0.9, 1.0, 0.97, 1.0)
MESH = pl.DeviceIdType.MESH


def broadcast(block, axis, owner):
    block = jnp.where(lax.axis_index(axis) == owner, block, jnp.zeros_like(block))
    return lax.psum(block, axis)


def noise_factors(kraus_rows):
    qubit_count = kraus_rows.shape[-1]
    register = 2**qubit_count
    positions = jnp.arange(register, dtype=jnp.int32)
    product = jnp.ones(kraus_rows.shape[:-1] + (register,), jnp.float32)
    for qubit_pos in range(qubit_count):
        bit_value = jnp.right_shift(positions, qubit_count - 1 - qubit_pos) & 1
        column = kraus_rows[..., qubit_pos : qubit_pos + 1]
        low_value = jnp.zeros(column.shape, jnp.float32)
        high_value = jnp.zeros(column.shape, jnp.float32)
        for option in range(4):
            picked = (column == option).astype(jnp.float32)
            low_value = low_value + picked * KEEP_FACTORS[option]
            high_value = high_value + picked * FLIP_FACTORS[option]
        product = product * jnp.where(bit_value == 1, high_value, low_value)
    return product


def apply_gate(amplitudes, matrix, factors, target):

    def on_low(values):
        mixed_rows = jnp.einsum("bhmk,ik->bhmi", values, matrix, precision=lax.Precision.HIGHEST)
        return mixed_rows * factors[:, None, None, :]

    def on_high(values):
        mixed_rows = jnp.einsum("bjmk,ij->bimk", values, matrix, precision=lax.Precision.HIGHEST)
        return mixed_rows * factors[:, :, None, None]

    return lax.cond(target == 0, on_low, on_high, amplitudes)


def square_sums(values):
    return (values, jnp.sum(values * values, axis=(1, 2, 3)))


def body(states, gate_blocks, kraus_picks, block_targets):
    traj_here = states.shape[0]
    amp_local = states.shape[1]
    register = gate_blocks.shape[-1]
    blocks = gate_blocks.shape[1]
    middle = amp_local // (register * register)
    total_amps = amp_local * lax.axis_size("amp")
    sections = lax.axis_size("segment")
    amplitudes = states.reshape(traj_here, register, middle, register)
    first_local = jnp.sum(amplitudes * amplitudes, axis=(1, 2, 3))
    local_sums = [first_local]
    for section in range(sections):
        section_gates = broadcast(gate_blocks, "segment", section)[0]
        for block_pos in range(blocks):
            factors = noise_factors(kraus_picks[:, section, block_pos, :])
            amplitudes = apply_gate(
                amplitudes, section_gates[block_pos], factors, block_targets[section, block_pos]
            )
        amplitudes, local_sq = square_sums(
            lax.all_to_all(amplitudes, "amp", split_axis=1, concat_axis=1, tiled=True)
        )
        local_sums.append(local_sq)
    totals = lax.psum(jnp.stack(local_sums, axis=1), "amp")
    log_weights = jnp.log(totals[:, 1:] / totals[:, :-1])
    amplitudes = amplitudes / jnp.sqrt(totals[:, -1] / total_amps)[:, None, None, None]
    return (amplitudes.reshape(traj_here, amp_local), log_weights)


def partner(index, k):
    result = index
    bit = 1
    while bit <= k:
        if k & bit:
            result = result + bit * (1 - 2 * ((index // bit) % 2))
        bit *= 2
    return result


def split(values):
    high = values.astype(jnp.bfloat16)
    low = (values - high.astype(jnp.float32)).astype(jnp.bfloat16)
    return high, low


def left_form(matrix):
    return jnp.concatenate(split(matrix), axis=1)


def right_form(matrix):
    row = jnp.concatenate(split(matrix), axis=1)
    return jnp.concatenate([row, row], axis=0)


def multiply(left, right):
    both = jnp.dot(left, right, preferred_element_type=jnp.float32)
    half = both.shape[1] // 2
    return both[:, :half] + both[:, half:]


def fold_rows(values):
    squares = values * values
    return jnp.sum(squares.reshape(-1, 8, squares.shape[-1]), axis=0)


def row_factors(picks_ref, section, block, qubits, shape):
    positions = lax.broadcasted_iota(jnp.int32, shape, 0)
    product = jnp.ones(shape, jnp.float32)
    for q in range(qubits):
        pick = picks_ref[0, block, section, q]
        keep = jnp.float32(KEEP_FACTORS[0])
        flip = jnp.float32(FLIP_FACTORS[0])
        for option in range(1, 4):
            keep = jnp.where(pick == option, jnp.float32(KEEP_FACTORS[option]), keep)
            flip = jnp.where(pick == option, jnp.float32(FLIP_FACTORS[option]), flip)
        bit = jnp.right_shift(positions, qubits - 1 - q) & 1
        product = product * jnp.where(bit == 1, flip, keep)
    return product


def circuit_kernel(
    peers, sections, blocks, qubits, chunks, total_amps,
    x_hbm, gates_hbm, picks_ref, targets_ref,
    out_ref, logs_ref,
    xs, yin, ov, gates, low_form, high_form, partial, sums,
    x_sem, own_sem, gate_sem, gsend, grecv, isend, irecv, osend, orecv, ssend, srecv,
):
    seg = lax.axis_index("segment")
    amp = lax.axis_index("amp")
    reg = gates.shape[-1]
    middle = chunks * peers
    order = list(range(peers - 1, 0, -1))

    loads = []
    for chunk in range(chunks):
        for d in range(peers):
            m = chunk * peers + d
            load = pltpu.make_async_copy(x_hbm.at[:, m, 0], xs.at[m], x_sem.at[m])
            load.start()
            loads.append(load)
    gate_load = pltpu.make_async_copy(gates_hbm, gates.at[seg], gate_sem)
    gate_load.start()
    own_loads = []
    for chunk in range(chunks):
        own = pltpu.make_async_copy(
            x_hbm.at[:, chunk * peers + amp, 0], yin.at[chunk, amp], own_sem.at[chunk]
        )
        own.start()
        own_loads.append(own)

    barrier = pltpu.get_barrier_semaphore()
    for k in order:
        pl.semaphore_signal(
            barrier, inc=1, device_id={"amp": partner(amp, k)}, device_id_type=MESH
        )
    for k in range(1, sections):
        pl.semaphore_signal(
            barrier, inc=1, device_id={"segment": partner(seg, k)}, device_id_type=MESH
        )
    pl.semaphore_wait(barrier, peers - 1 + sections - 1)

    for load in loads:
        load.wait()

    in_copies = []
    for chunk in range(chunks):
        copies = []
        for k in order:
            peer = partner(amp, k)
            copy = pltpu.make_async_remote_copy(
                src_ref=xs.at[chunk * peers + peer],
                dst_ref=yin.at[chunk, amp],
                send_sem=isend.at[chunk, k],
                recv_sem=irecv.at[chunk, k],
                device_id={"amp": peer},
                device_id_type=MESH,
            )
            copy.start()
            copies.append(copy)
        in_copies.append(copies)

    gate_load.wait()
    gate_copies = []
    for k in range(1, sections):
        copy = pltpu.make_async_remote_copy(
            src_ref=gates.at[seg],
            dst_ref=gates.at[seg],
            send_sem=gsend.at[k],
            recv_sem=grecv.at[k],
            device_id={"segment": partner(seg, k)},
            device_id_type=MESH,
        )
        copy.start()
        gate_copies.append(copy)
    for copy in gate_copies:
        copy.wait_recv()

    rows_at = lax.broadcasted_iota(jnp.int32, (reg, reg), 0)
    columns_at = lax.broadcasted_iota(jnp.int32, (reg, reg), 1)
    identity = jnp.where(rows_at == columns_at, jnp.float32(1.0), jnp.float32(0.0))

    def build(section, carry):
        low = high = None
        for b in range(blocks):
            factors = row_factors(picks_ref, section, b, qubits, (reg, reg))
            damped = gates[section, b] * factors
            is_low = targets_ref[section, b] == 0
            for_low = jnp.where(is_low, damped, identity)
            for_high = jnp.where(is_low, identity, damped)
            if b == 0:
                low, high = for_low, for_high
            else:
                low = multiply(left_form(for_low), right_form(low))
                high = multiply(left_form(for_high), right_form(high))
        low_form[section] = right_form(low.T)
        high_form[section] = left_form(high)
        return carry

    lax.fori_loop(0, sections, build, 0)

    inner = reg // peers
    partial[...] = jnp.zeros_like(partial)

    def apply_section(chunk, section, swapped):
        low = low_form[section]
        high = high_form[section]
        total = jnp.zeros((8, reg), jnp.float32)
        for slab in range(peers):
            if swapped:
                value = yin[chunk, :, slab * inner : (slab + 1) * inner, :].reshape(reg, reg)
            else:
                value = yin[chunk, slab]
            value = multiply(left_form(value), low)
            value = multiply(high, right_form(value))
            total = total + fold_rows(value)
            if swapped:
                yin[chunk, :, slab * inner : (slab + 1) * inner, :] = value.reshape(
                    peers, inner, reg
                )
            else:
                yin[chunk, slab] = value
        partial[section + 1] = partial[section + 1] + total

    out_copies = []
    for chunk in range(chunks):
        own_loads[chunk].wait()
        for copy in in_copies[chunk]:
            copy.wait_recv()
        first = jnp.zeros((8, reg), jnp.float32)
        for slab in range(peers):
            first = first + fold_rows(yin[chunk, slab])
        partial[0] = partial[0] + first

        def pair(i, carry, chunk=chunk):
            apply_section(chunk, 2 * i, False)
            apply_section(chunk, 2 * i + 1, True)
            return carry

        lax.fori_loop(0, sections // 2, pair, 0)

        if chunk == chunks - 1:
            for s in range(sections + 1):
                sums[amp, s : s + 1, :] = jnp.sum(partial[s], axis=0, keepdims=True)
            sum_copies = []
            for k in order:
                copy = pltpu.make_async_remote_copy(
                    src_ref=sums.at[amp],
                    dst_ref=sums.at[amp],
                    send_sem=ssend.at[k],
                    recv_sem=srecv.at[k],
                    device_id={"amp": partner(amp, k)},
                    device_id_type=MESH,
                )
                copy.start()
                sum_copies.append(copy)
        copies = []
        for k in order:
            peer = partner(amp, k)
            copy = pltpu.make_async_remote_copy(
                src_ref=yin.at[chunk, peer],
                dst_ref=ov.at[chunk, amp],
                send_sem=osend.at[chunk, k],
                recv_sem=orecv.at[chunk, k],
                device_id={"amp": peer},
                device_id_type=MESH,
            )
            copy.start()
            copies.append(copy)
        out_copies.append(copies)

    for copy in sum_copies:
        copy.wait_recv()
    totals = []
    for s in range(sections + 1):
        total = sums[0, s : s + 1, :]
        for d in range(1, peers):
            total = total + sums[d, s : s + 1, :]
        totals.append(jnp.sum(total, axis=1, keepdims=True))
    lanes = lax.broadcasted_iota(jnp.int32, (1, reg), 1)
    logs = jnp.zeros((1, reg), jnp.float32)
    for s in range(sections):
        logs = jnp.where(lanes == s, jnp.log(totals[s + 1] / totals[s]), logs)
    logs_ref[...] = logs[:, :sections]
    scale = 1.0 / jnp.sqrt(totals[sections] / total_amps)
    scale = jnp.broadcast_to(scale, (1, reg))

    for chunk in range(chunks):
        m = chunk * peers + amp
        out_ref[pl.ds(m, reg, stride=middle), :] = yin[chunk, amp] * scale
    for chunk in range(chunks):
        for at, k in reversed(list(enumerate(order))):
            out_copies[chunk][at].wait_recv()
            m = chunk * peers + partner(amp, k)
            out_ref[pl.ds(m, reg, stride=middle), :] = ov[chunk, partner(amp, k)] * scale

    for copies in in_copies + out_copies + [gate_copies, sum_copies]:
        for copy in copies:
            copy.wait_send()


def step(states, gate_blocks, kraus_picks, block_targets):
    traj_here, amp_local = states.shape
    reg = gate_blocks.shape[-1]
    blocks = gate_blocks.shape[1]
    qubits = kraus_picks.shape[-1]
    peers = lax.axis_size("amp")
    sections = lax.axis_size("segment")
    middle = amp_local // (reg * reg)
    fits = (
        traj_here == 1
        and gate_blocks.shape[0] == 1
        and middle % peers == 0
        and peers & (peers - 1) == 0
        and sections & (sections - 1) == 0
        and sections % 2 == 0
        and sections < 8
        and reg == 128
        and reg % (8 * peers) == 0
    )
    if not fits:
        return body(states, gate_blocks, kraus_picks, block_targets)
    chunks = middle // peers
    kernel = functools.partial(
        circuit_kernel, peers, sections, blocks, qubits, chunks, amp_local * peers
    )
    f32 = jnp.float32
    dma = pltpu.SemaphoreType.DMA
    out, logs = pl.pallas_call(
        kernel,
        out_shape=(
            pltpu.VMEM((reg * middle, reg), f32),
            pltpu.VMEM((1, sections), f32),
        ),
        in_specs=[
            pl.BlockSpec(memory_space=pl.ANY),
            pl.BlockSpec(memory_space=pl.ANY),
            pl.BlockSpec(memory_space=pltpu.SMEM),
            pl.BlockSpec(memory_space=pltpu.SMEM),
        ],
        out_specs=(
            pl.BlockSpec(memory_space=pltpu.VMEM),
            pl.BlockSpec(memory_space=pltpu.VMEM),
        ),
        scratch_shapes=[
            pltpu.VMEM((middle, reg, reg), f32),
            pltpu.VMEM((chunks, peers, reg, reg), f32),
            pltpu.VMEM((chunks, peers, reg, reg), f32),
            pltpu.VMEM((sections, blocks, reg, reg), f32),
            pltpu.VMEM((sections, 2 * reg, 2 * reg), jnp.bfloat16),
            pltpu.VMEM((sections, reg, 2 * reg), jnp.bfloat16),
            pltpu.VMEM((sections + 1, 8, reg), f32),
            pltpu.VMEM((peers, 8, reg), f32),
            dma((middle,)),
            dma((chunks,)),
            dma,
            dma((sections,)),
            dma((sections,)),
            dma((chunks, peers)),
            dma((chunks, peers)),
            dma((chunks, peers)),
            dma((chunks, peers)),
            dma((peers,)),
            dma((peers,)),
        ],
        compiler_params=pltpu.CompilerParams(collective_id=0, has_side_effects=True),
    )(
        states.reshape(reg, middle, 1, reg),
        gate_blocks[0],
        jnp.swapaxes(kraus_picks, 1, 2),
        block_targets,
    )
    return out.reshape(1, amp_local), logs


def solution(mesh):
    in_specs = (
        P("segment", "amp"),
        P("segment", None, None, None),
        P("segment", None, None, None),
        P(),
    )
    out_specs = (P("segment", "amp"), P("segment", None))
    return jax.shard_map(step, mesh=mesh, in_specs=in_specs, out_specs=out_specs, check_vma=False)
```

```python
import functools

import jax
import jax.numpy as jnp
from jax import lax
from jax.experimental import pallas as pl
from jax.experimental.pallas import tpu as pltpu
from jax.sharding import PartitionSpec as P

KEEP_FACTORS = (1.0, 0.9, 1.0, 0.97)
FLIP_FACTORS = (0.9, 1.0, 0.97, 1.0)
MESH = pl.DeviceIdType.MESH


def broadcast(block, axis, owner):
    block = jnp.where(lax.axis_index(axis) == owner, block, jnp.zeros_like(block))
    return lax.psum(block, axis)


def noise_factors(kraus_rows):
    qubit_count = kraus_rows.shape[-1]
    register = 2**qubit_count
    positions = jnp.arange(register, dtype=jnp.int32)
    product = jnp.ones(kraus_rows.shape[:-1] + (register,), jnp.float32)
    for qubit_pos in range(qubit_count):
        bit_value = jnp.right_shift(positions, qubit_count - 1 - qubit_pos) & 1
        column = kraus_rows[..., qubit_pos : qubit_pos + 1]
        low_value = jnp.zeros(column.shape, jnp.float32)
        high_value = jnp.zeros(column.shape, jnp.float32)
        for option in range(4):
            picked = (column == option).astype(jnp.float32)
            low_value = low_value + picked * KEEP_FACTORS[option]
            high_value = high_value + picked * FLIP_FACTORS[option]
        product = product * jnp.where(bit_value == 1, high_value, low_value)
    return product


def apply_gate(amplitudes, matrix, factors, target):

    def on_low(values):
        mixed_rows = jnp.einsum("bhmk,ik->bhmi", values, matrix, precision=lax.Precision.HIGHEST)
        return mixed_rows * factors[:, None, None, :]

    def on_high(values):
        mixed_rows = jnp.einsum("bjmk,ij->bimk", values, matrix, precision=lax.Precision.HIGHEST)
        return mixed_rows * factors[:, :, None, None]

    return lax.cond(target == 0, on_low, on_high, amplitudes)


def square_sums(values):
    return (values, jnp.sum(values * values, axis=(1, 2, 3)))


def body(states, gate_blocks, kraus_picks, block_targets):
    traj_here = states.shape[0]
    amp_local = states.shape[1]
    register = gate_blocks.shape[-1]
    blocks = gate_blocks.shape[1]
    middle = amp_local // (register * register)
    total_amps = amp_local * lax.axis_size("amp")
    sections = lax.axis_size("segment")
    amplitudes = states.reshape(traj_here, register, middle, register)
    first_local = jnp.sum(amplitudes * amplitudes, axis=(1, 2, 3))
    local_sums = [first_local]
    for section in range(sections):
        section_gates = broadcast(gate_blocks, "segment", section)[0]
        for block_pos in range(blocks):
            factors = noise_factors(kraus_picks[:, section, block_pos, :])
            amplitudes = apply_gate(
                amplitudes, section_gates[block_pos], factors, block_targets[section, block_pos]
            )
        amplitudes, local_sq = square_sums(
            lax.all_to_all(amplitudes, "amp", split_axis=1, concat_axis=1, tiled=True)
        )
        local_sums.append(local_sq)
    totals = lax.psum(jnp.stack(local_sums, axis=1), "amp")
    log_weights = jnp.log(totals[:, 1:] / totals[:, :-1])
    amplitudes = amplitudes / jnp.sqrt(totals[:, -1] / total_amps)[:, None, None, None]
    return (amplitudes.reshape(traj_here, amp_local), log_weights)


def partner(index, k):
    result = index
    bit = 1
    while bit <= k:
        if k & bit:
            result = result + bit * (1 - 2 * ((index // bit) % 2))
        bit *= 2
    return result


def split(values):
    high = values.astype(jnp.bfloat16)
    low = (values - high.astype(jnp.float32)).astype(jnp.bfloat16)
    return high, low


def left_form(matrix):
    return jnp.concatenate(split(matrix), axis=1)


def right_form(matrix):
    row = jnp.concatenate(split(matrix), axis=1)
    return jnp.concatenate([row, row], axis=0)


def multiply(left, right):
    both = jnp.dot(left, right, preferred_element_type=jnp.float32)
    half = both.shape[1] // 2
    return both[:, :half] + both[:, half:]


def fold_rows(values):
    squares = values * values
    return jnp.sum(squares.reshape(-1, 8, squares.shape[-1]), axis=0)


def row_factors(picks_ref, section, block, qubits, shape):
    positions = lax.broadcasted_iota(jnp.int32, shape, 0)
    product = jnp.ones(shape, jnp.float32)
    for q in range(qubits):
        pick = picks_ref[0, block, section, q]
        keep = jnp.float32(KEEP_FACTORS[0])
        flip = jnp.float32(FLIP_FACTORS[0])
        for option in range(1, 4):
            keep = jnp.where(pick == option, jnp.float32(KEEP_FACTORS[option]), keep)
            flip = jnp.where(pick == option, jnp.float32(FLIP_FACTORS[option]), flip)
        bit = jnp.right_shift(positions, qubits - 1 - q) & 1
        product = product * jnp.where(bit == 1, flip, keep)
    return product


def circuit_kernel(
    peers, sections, blocks, qubits, chunks, total_amps,
    x_hbm, gates_hbm, picks_ref, targets_ref,
    out_ref, logs_ref,
    xs, yin, ov, gates, low_form, high_form, partial, sums,
    x_sem, own_sem, gate_sem, gsend, grecv, isend, irecv, osend, orecv, ssend, srecv,
    entered,
):
    seg = lax.axis_index("segment")
    amp = lax.axis_index("amp")
    reg = gates.shape[-1]
    middle = chunks * peers
    order = list(range(peers - 1, 0, -1))

    loads = []
    for chunk in range(chunks):
        for d in range(peers):
            m = chunk * peers + d
            load = pltpu.make_async_copy(x_hbm.at[:, m, 0], xs.at[m], x_sem.at[m])
            load.start()
            loads.append(load)
    gate_load = pltpu.make_async_copy(gates_hbm, gates.at[seg], gate_sem)
    gate_load.start()
    own_loads = []
    for chunk in range(chunks):
        own = pltpu.make_async_copy(
            x_hbm.at[:, chunk * peers + amp, 0], yin.at[chunk, amp], own_sem.at[chunk]
        )
        own.start()
        own_loads.append(own)

    in_copies = []
    for chunk in range(chunks):
        copies = {}
        for k in order:
            peer = partner(amp, k)
            copies[k] = pltpu.make_async_remote_copy(
                src_ref=xs.at[chunk * peers + peer],
                dst_ref=yin.at[chunk, amp],
                send_sem=isend.at[chunk, k],
                recv_sem=irecv.at[chunk, k],
                device_id={"amp": peer},
                device_id_type=MESH,
            )
        in_copies.append(copies)

    def tell(semaphore, axis, index, k):
        pl.semaphore_signal(
            semaphore, inc=1, device_id={axis: partner(index, k)}, device_id_type=MESH
        )

    barrier = pltpu.get_barrier_semaphore()
    if peers == 8 and sections == 4:
        pair_at = amp // 2
        inner_pair = (pair_at + 1) // 2 % 2
        is_inner = inner_pair == 1
        for k in (1, 2):
            tell(barrier, "segment", seg, k)
        for k in (1, 2, 3):
            tell(barrier, "amp", amp, k)

        @pl.when(is_inner)
        def _():
            tell(barrier, "amp", amp, 6)
            tell(barrier, "amp", amp, 7)

        for load in loads:
            load.wait()
        pl.semaphore_wait(barrier, 5 + 2 * inner_pair)

        @pl.when(is_inner)
        def _():
            tell(entered.at[0], "amp", amp, 2)
            tell(entered.at[0], "amp", amp, 6)
            in_copies[0][6].start()
            in_copies[0][7].start()

        tell(entered.at[2], "segment", seg, 1)
        pl.semaphore_wait(entered.at[0], 1)

        @pl.when(is_inner)
        def _():
            tell(entered.at[1], "amp", amp, 2)

        in_copies[0][4].start()
        in_copies[0][5].start()

        @pl.when(jnp.logical_not(is_inner))
        def _():
            pl.semaphore_wait(entered.at[1], 1)
            in_copies[0][6].start()
            in_copies[0][7].start()

        for k in (3, 2, 1):
            in_copies[0][k].start()
        rest = in_copies[1:]
        pl.semaphore_wait(entered.at[2], 1)
    else:
        for k in order:
            tell(barrier, "amp", amp, k)
        for k in range(1, sections):
            tell(barrier, "segment", seg, k)
        for load in loads:
            load.wait()
        pl.semaphore_wait(barrier, peers - 1 + sections - 1)
        rest = in_copies
    for copies in rest:
        for k in order:
            copies[k].start()
    in_copies = [list(copies.values()) for copies in in_copies]

    gate_load.wait()
    gate_copies = []
    for k in range(1, sections):
        copy = pltpu.make_async_remote_copy(
            src_ref=gates.at[seg],
            dst_ref=gates.at[seg],
            send_sem=gsend.at[k],
            recv_sem=grecv.at[k],
            device_id={"segment": partner(seg, k)},
            device_id_type=MESH,
        )
        copy.start()
        gate_copies.append(copy)
    for copy in gate_copies:
        copy.wait_recv()

    rows_at = lax.broadcasted_iota(jnp.int32, (reg, reg), 0)
    columns_at = lax.broadcasted_iota(jnp.int32, (reg, reg), 1)
    identity = jnp.where(rows_at == columns_at, jnp.float32(1.0), jnp.float32(0.0))

    def build(section, carry):
        low = high = None
        for b in range(blocks):
            factors = row_factors(picks_ref, section, b, qubits, (reg, reg))
            damped = gates[section, b] * factors
            is_low = targets_ref[section, b] == 0
            for_low = jnp.where(is_low, damped, identity)
            for_high = jnp.where(is_low, identity, damped)
            if b == 0:
                low, high = for_low, for_high
            else:
                low = multiply(left_form(for_low), right_form(low))
                high = multiply(left_form(for_high), right_form(high))
        low_form[section] = right_form(low.T)
        high_form[section] = left_form(high)
        return carry

    lax.fori_loop(0, sections, build, 0)

    inner = reg // peers
    partial[...] = jnp.zeros_like(partial)

    def apply_section(chunk, section, swapped):
        low = low_form[section]
        high = high_form[section]
        total = jnp.zeros((8, reg), jnp.float32)
        for slab in range(peers):
            if swapped:
                value = yin[chunk, :, slab * inner : (slab + 1) * inner, :].reshape(reg, reg)
            else:
                value = yin[chunk, slab]
            value = multiply(left_form(value), low)
            value = multiply(high, right_form(value))
            total = total + fold_rows(value)
            if swapped:
                yin[chunk, :, slab * inner : (slab + 1) * inner, :] = value.reshape(
                    peers, inner, reg
                )
            else:
                yin[chunk, slab] = value
        partial[section + 1] = partial[section + 1] + total

    out_copies = []
    order_out = [5, 4, 7, 6, 3, 2, 1]
    for chunk in range(chunks):
        own_loads[chunk].wait()
        for copy in in_copies[chunk]:
            copy.wait_recv()
        first = jnp.zeros((8, reg), jnp.float32)
        for slab in range(peers):
            first = first + fold_rows(yin[chunk, slab])
        partial[0] = partial[0] + first

        def pair(i, carry, chunk=chunk):
            apply_section(chunk, 2 * i, False)
            apply_section(chunk, 2 * i + 1, True)
            return carry

        lax.fori_loop(0, sections // 2, pair, 0)

        if chunk == chunks - 1:
            for s in range(sections + 1):
                sums[amp, s : s + 1, :] = jnp.sum(partial[s], axis=0, keepdims=True)
            sum_copies = []
            for k in order:
                copy = pltpu.make_async_remote_copy(
                    src_ref=sums.at[amp],
                    dst_ref=sums.at[amp],
                    send_sem=ssend.at[k],
                    recv_sem=srecv.at[k],
                    device_id={"amp": partner(amp, k)},
                    device_id_type=MESH,
                )
                copy.start()
                sum_copies.append(copy)
        copies = []
        for k in order_out:
            peer = partner(amp, k)
            copy = pltpu.make_async_remote_copy(
                src_ref=yin.at[chunk, peer],
                dst_ref=ov.at[chunk, amp],
                send_sem=osend.at[chunk, k],
                recv_sem=orecv.at[chunk, k],
                device_id={"amp": peer},
                device_id_type=MESH,
            )
            copy.start()
            copies.append(copy)
        out_copies.append(copies)

    for copy in sum_copies:
        copy.wait_recv()
    totals = []
    for s in range(sections + 1):
        total = sums[0, s : s + 1, :]
        for d in range(1, peers):
            total = total + sums[d, s : s + 1, :]
        totals.append(jnp.sum(total, axis=1, keepdims=True))
    lanes = lax.broadcasted_iota(jnp.int32, (1, reg), 1)
    logs = jnp.zeros((1, reg), jnp.float32)
    for s in range(sections):
        logs = jnp.where(lanes == s, jnp.log(totals[s + 1] / totals[s]), logs)
    logs_ref[...] = logs[:, :sections]
    scale = 1.0 / jnp.sqrt(totals[sections] / total_amps)
    scale = jnp.broadcast_to(scale, (1, reg))

    for chunk in range(chunks):
        m = chunk * peers + amp
        out_ref[pl.ds(m, reg, stride=middle), :] = yin[chunk, amp] * scale
    for chunk in range(chunks):
        for at, k in reversed(list(enumerate(order_out))):
            out_copies[chunk][at].wait_recv()
            m = chunk * peers + partner(amp, k)
            out_ref[pl.ds(m, reg, stride=middle), :] = ov[chunk, partner(amp, k)] * scale

    for copies in in_copies + out_copies + [gate_copies, sum_copies]:
        for copy in copies:
            copy.wait_send()


def step(states, gate_blocks, kraus_picks, block_targets):
    traj_here, amp_local = states.shape
    reg = gate_blocks.shape[-1]
    blocks = gate_blocks.shape[1]
    qubits = kraus_picks.shape[-1]
    peers = lax.axis_size("amp")
    sections = lax.axis_size("segment")
    middle = amp_local // (reg * reg)
    fits = (
        traj_here == 1
        and gate_blocks.shape[0] == 1
        and middle % peers == 0
        and peers & (peers - 1) == 0
        and sections & (sections - 1) == 0
        and sections % 2 == 0
        and sections < 8
        and reg == 128
        and reg % (8 * peers) == 0
    )
    if not fits:
        return body(states, gate_blocks, kraus_picks, block_targets)
    chunks = middle // peers
    kernel = functools.partial(
        circuit_kernel, peers, sections, blocks, qubits, chunks, amp_local * peers
    )
    f32 = jnp.float32
    dma = pltpu.SemaphoreType.DMA
    out, logs = pl.pallas_call(
        kernel,
        out_shape=(
            pltpu.VMEM((reg * middle, reg), f32),
            pltpu.VMEM((1, sections), f32),
        ),
        in_specs=[
            pl.BlockSpec(memory_space=pl.ANY),
            pl.BlockSpec(memory_space=pl.ANY),
            pl.BlockSpec(memory_space=pltpu.SMEM),
            pl.BlockSpec(memory_space=pltpu.SMEM),
        ],
        out_specs=(
            pl.BlockSpec(memory_space=pltpu.VMEM),
            pl.BlockSpec(memory_space=pltpu.VMEM),
        ),
        scratch_shapes=[
            pltpu.VMEM((middle, reg, reg), f32),
            pltpu.VMEM((chunks, peers, reg, reg), f32),
            pltpu.VMEM((chunks, peers, reg, reg), f32),
            pltpu.VMEM((sections, blocks, reg, reg), f32),
            pltpu.VMEM((sections, 2 * reg, 2 * reg), jnp.bfloat16),
            pltpu.VMEM((sections, reg, 2 * reg), jnp.bfloat16),
            pltpu.VMEM((sections + 1, 8, reg), f32),
            pltpu.VMEM((peers, 8, reg), f32),
            dma((middle,)),
            dma((chunks,)),
            dma,
            dma((sections,)),
            dma((sections,)),
            dma((chunks, peers)),
            dma((chunks, peers)),
            dma((chunks, peers)),
            dma((chunks, peers)),
            dma((peers,)),
            dma((peers,)),
            pltpu.SemaphoreType.REGULAR((3,)),
        ],
        compiler_params=pltpu.CompilerParams(collective_id=0, has_side_effects=True),
    )(
        states.reshape(reg, middle, 1, reg),
        gate_blocks[0],
        jnp.swapaxes(kraus_picks, 1, 2),
        block_targets,
    )
    return out.reshape(1, amp_local), logs


def solution(mesh):
    in_specs = (
        P("segment", "amp"),
        P("segment", None, None, None),
        P("segment", None, None, None),
        P(),
    )
    out_specs = (P("segment", "amp"), P("segment", None))
    return jax.shard_map(step, mesh=mesh, in_specs=in_specs, out_specs=out_specs, check_vma=False)
```
